16 devices in a mesh: dp: 4 (over y, z, core), tp: 4 (over x).
Axes of the slice: x: 4, y: 2, z: 1, core: 2. Of those that a mesh axis runs over, the one named last changes fastest.
The devices are a block of a 4x4x8 slice.
Arguments:
- x: bfloat16 [8192, 7168], P('dp'), parts along dimension 0
- gain: bfloat16 [7168], replicated
- wq: bfloat16 [7168, 7168], P(None, 'tp')
- wk: bfloat16 [7168, 1024], P(None, 'tp')
- wv: bfloat16 [7168, 1024], P(None, 'tp')
- wo: bfloat16 [7168, 7168], P('tp')
Outputs:
- output: bfloat16 [8192, 7168], P('dp'), parts along dimension 0
There are 4 independent parts. The reference program is written for one: setup_inputs(seed, part) draws one part's arguments, and reference() takes and returns one part's arrays. A program takes and returns all parts, laid end to end along the dimension named above; an argument that names none is the same for every part.
All inputs are finite; a program needn't handle non-finite values.
Results may differ from the reference program's by a relative error of at most 0.012.
Values are sent between devices in bfloat16 or wider.
A program may use at most 768 MiB of HBM per device.

```python
import jax
import jax.numpy as jnp
from jax import lax

ROWS = 2048
D = 7168
HEADS = 56
KV_HEADS = 8
HEAD = 128
THETA = 10000


def setup_inputs(seed: int = 0, part: int = 0) -> dict:
    kx, kn, kq, kk, kv, ko = jax.random.split(jax.random.key(seed), 6)

    def weights(key, rows, columns):
        return jax.random.normal(key, (rows, columns), jnp.float32) * rows**-0.5

    drawn = {
        "x": jax.random.normal(jax.random.fold_in(kx, part), (ROWS, D), jnp.float32),
        "gain": 1 + 0.1 * jax.random.normal(kn, (D,), jnp.float32),
        "wq": 2 * weights(kq, D, HEADS * HEAD),
        "wk": 2 * weights(kk, D, KV_HEADS * HEAD),
        "wv": 4 * weights(kv, D, KV_HEADS * HEAD),
        "wo": weights(ko, HEADS * HEAD, D),
    }
    return {k: v.astype(jnp.bfloat16) for k, v in drawn.items()}


def normed(x, gain):
    wide = x.astype(jnp.float32)
    scale = lax.rsqrt(jnp.mean(wide * wide, -1, keepdims=True) + 1e-6)
    return (wide * scale * gain.astype(jnp.float32)).astype(jnp.bfloat16)


def turned(t, place, theta):
    half = t.shape[-1] // 2
    angle = place.astype(jnp.float32)[:, None] * theta ** (-jnp.arange(half, dtype=jnp.float32) / half)
    cos, sin = jnp.cos(angle)[:, None], jnp.sin(angle)[:, None]
    a, b = t[..., :half].astype(jnp.float32), t[..., half:].astype(jnp.float32)
    return jnp.concatenate([a * cos - b * sin, b * cos + a * sin], -1).astype(jnp.bfloat16)


def matmul(a, w):
    return jnp.dot(a, w, preferred_element_type=jnp.float32).astype(jnp.bfloat16)


def einsum(form, a, b):
    return jnp.einsum(form, a.astype(jnp.float32), b.astype(jnp.float32))


def attention(q, k, v):
    scores = einsum("tgsd,ugd->gstu", q, k) * q.shape[-1] ** -0.5
    token = jnp.arange(q.shape[0])
    scores = jnp.where(token[:, None] >= token, scores, -jnp.inf)
    weights = jax.nn.softmax(scores, -1).astype(jnp.bfloat16)
    return einsum("gstu,ugd->tgsd", weights, v).astype(jnp.bfloat16)


def reference(x, gain, wq, wk, wv, wo):
    a, place = normed(x, gain), jnp.arange(ROWS)
    q = turned(matmul(a, wq).reshape(ROWS, HEADS, HEAD), place, THETA).reshape(ROWS, KV_HEADS, -1, HEAD)
    k = turned(matmul(a, wk).reshape(ROWS, KV_HEADS, HEAD), place, THETA)
    v = matmul(a, wv).reshape(ROWS, KV_HEADS, HEAD)
    seen = attention(q, k, v).reshape(ROWS, HEADS * HEAD)
    return (x.astype(jnp.float32) + jnp.dot(seen, wo, preferred_element_type=jnp.float32)).astype(jnp.bfloat16)
```

```python
import functools

import jax
import jax.numpy as jnp
from jax import lax
from jax.experimental import pallas as pl
from jax.experimental.pallas import tpu as pltpu
from jax.sharding import PartitionSpec as P

HEAD = 128
THETA = 10000
T = 256
WB = 256
NEG = -1e30
HIDDEN = 2 * NEG
LOG2E = 1.4426950408889634
VMEM = 67_000_000
RING = 4


def _dot(a, b, ca, cb):
    return lax.dot_general(a, b, (((ca,), (cb,)), ((), ())), preferred_element_type=jnp.float32)


def _layer(x, gain, cs, wq, wk, wv, wo, y, x_s, a_s, cs_s, w_s, wo_s, q_s, k_s, v_s, seen_s, top_s, mix_s, out_s, relay_s, fin_s, got_s,
           term_s, xr_s, x_sem, cs_sem, w_sem, wo_sem, xr_sem, l_sem, s_sem, r_sem):
    rows, depth = x.shape
    chunks = rows // T
    heads, kv = q_s.shape[0], k_s.shape[1]
    group = heads // kv
    width = wo_s.shape[2]
    nq = wq.shape[1] // WB
    nb = nq + 2
    first = (nb + 1) // 2
    me = lax.axis_index("tp")
    right, left = lax.rem(me + 1, RING), lax.rem(me + 3, RING)

    def at_rows(p):
        return pl.ds(pl.multiple_of(p * T, T), T)

    def at_cols(hp):
        return pl.ds(pl.multiple_of(hp * width, 128), width)

    def remote(kind, slot, src, dst, to):
        return pltpu.make_async_remote_copy(src_ref=src, dst_ref=dst, send_sem=s_sem.at[kind], recv_sem=r_sem.at[slot, kind],
                                            device_id={"tp": to}, device_id_type=pl.DeviceIdType.MESH)

    def small(kind, slot):
        return remote(kind, slot, out_s.at[0], got_s.at[0, 0], right)

    def load_x(p):
        return pltpu.make_async_copy(x.at[at_rows(p), :], x_s, x_sem)

    def load_cs(p):
        return pltpu.make_async_copy(cs.at[:, at_rows(p), :], cs_s, cs_sem)

    def load_xr(p, h):
        return pltpu.make_async_copy(x.at[at_rows(p), at_cols(2 * me + h)], xr_s.at[h], xr_sem.at[h])

    def load_q(b, slot):
        return pltpu.make_async_copy(wq.at[:, pl.ds(pl.multiple_of(b * WB, WB), WB)], w_s.at[slot], w_sem.at[slot])

    def load_kv(w, slot):
        return pltpu.make_async_copy(w, w_s.at[slot], w_sem.at[slot])

    def load_wo(hp):
        return pltpu.make_async_copy(wo.at[:, at_cols(hp)], wo_s.at[hp], wo_sem.at[hp])

    def sent_half(m):
        off = 2 + (m // 2) * (2 * (m % 2) - 1)
        return 2 * lax.rem(me + off, RING) + lax.rem(m % 2 + m // 2, 2)

    def kept_half(m):
        off = (1 - m // 2) * (1 + 2 * (m % 2))
        return 2 * lax.rem(me + off, RING) + m % 2

    def norm():
        def some(r, _):
            here = pl.ds(pl.multiple_of(r * 16, 16), 16)
            wide = x_s[here, :].astype(jnp.float32)
            scale = lax.rsqrt(jnp.sum(wide * wide, -1, keepdims=True) / depth + 1e-6)
            a_s[here, :] = (wide * scale * gain[...].astype(jnp.float32)).astype(jnp.bfloat16)
            return None

        lax.fori_loop(0, T // 16, some, None)

    def project(slot):
        load_kv(wk, slot).wait()
        return _dot(a_s[...], w_s[slot], 1, 0).astype(jnp.bfloat16)

    def turn(t):
        wide = t.astype(jnp.float32)
        return (wide * cs_s[0] + pltpu.roll(wide, HEAD // 2, 1) * cs_s[1]).astype(jnp.bfloat16)

    def queries(c):
        def block(b, _):
            slot = lax.rem(c * nb + b, 2)
            t = project(slot)
            for i in range(WB // HEAD):
                q_s[b * (WB // HEAD) + i] = turn(t[:, i * HEAD : (i + 1) * HEAD])

            @pl.when(b + 2 < nq)
            def _():
                load_q(b + 2, slot).start()

            @pl.when(b + 2 == nq)
            def _():
                load_kv(wk, slot).start()

            @pl.when(b + 2 == nq + 1)
            def _():
                load_kv(wv, slot).start()

            return None

        return block

    def project_first(c):
        load_x(c).wait()
        norm()

        @pl.when(c + 1 < chunks)
        def _():
            load_x(c + 1).start()

        load_cs(c).wait()
        lax.fori_loop(0, first, queries(c), None)

    def project_rest(c):
        lax.fori_loop(first, nq, queries(c), None)
        slot = lax.rem(c * nb + nq, 2)
        t = project(slot)
        for i in range(kv):
            k_s[c, i] = turn(t[:, i * HEAD : (i + 1) * HEAD])

        @pl.when(c + 1 < chunks)
        def _():
            load_q(0, slot).start()
            load_cs(c + 1).start()

        slot = lax.rem(c * nb + nq + 1, 2)
        t = project(slot)
        for i in range(kv):
            v_s[c, i, :HEAD, :] = t[:, i * HEAD : (i + 1) * HEAD].T
            v_s[c, i, HEAD:, :] = jnp.ones((v_s.shape[2] - HEAD, T), jnp.bfloat16)

        @pl.when(c + 1 < chunks)
        def _():
            load_q(1, slot).start()

    def attention(c):
        e = HEAD**-0.5 * LOG2E
        top_s[...] = jnp.full(top_s.shape, NEG, jnp.float32)
        mix_s[...] = jnp.zeros(mix_s.shape, jnp.float32)
        ok = lax.broadcasted_iota(jnp.int32, (T, T), 0) <= lax.broadcasted_iota(jnp.int32, (T, T), 1)

        def block(j, masked):
            for i in range(kv):
                mine = range(i * group, (i + 1) * group)
                scores = [_dot(k_s[j, i], q_s[h], 1, 1) for h in mine]
                weights, keeps = [], []
                for h, s in zip(mine, scores):
                    if masked:
                        s = jnp.where(ok, s, HIDDEN)
                    old = top_s[h : h + 1, :]
                    top = jnp.maximum(old, s.max(axis=0, keepdims=True))
                    top_s[h : h + 1, :] = top
                    weights.append(jnp.exp2((s - top) * e).astype(jnp.bfloat16))
                    keeps.append(jnp.exp2((old - top) * e))
                for h, p, keep in zip(mine, weights, keeps):
                    mix_s[h] = mix_s[h] * keep + _dot(v_s[j, i], p, 1, 0)

        def whole(j, _):
            block(j, False)
            return None

        lax.fori_loop(0, c, whole, None)
        block(c, True)
        for h in range(heads):
            seen_s[:, h * HEAD : (h + 1) * HEAD] = (mix_s[h, :HEAD, :] * (1 / mix_s[h, HEAD : HEAD + 1, :])).T.astype(jnp.bfloat16)

    def term(p, hp):
        @pl.when(p == 0)
        def _():
            load_wo(hp).wait()

        return _dot(seen_s[...], wo_s[hp], 1, 0)

    def send_terms(p):
        slot = lax.rem(p, 2)

        def one(m, _):
            @pl.when(p >= 1)
            def _():
                small(m, slot).wait_send()

            out_s[m] = term(p, sent_half(m)).astype(jnp.bfloat16)
            remote(m, slot, out_s.at[m], got_s.at[slot, m], lax.rem(me + 1 + 2 * (m % 2), RING)).start()
            return None

        lax.fori_loop(0, 4, one, None)

    def keep_terms(p):
        def one(m, _):
            term_s[m] = term(p, kept_half(m))
            return None

        lax.fori_loop(0, 4, one, None)

    def relay(p):
        slot = lax.rem(p, 2)

        @pl.when(p >= 2)
        def _():
            for kind in range(8, 12):
                small(kind, slot).wait_recv()

        for d, to in ((0, right), (1, left)):

            @pl.when(p >= 1)
            def _():
                small(4 + d, slot).wait_send()

            small(d, slot).wait_recv()
            relay_s[d] = (got_s[slot, d].astype(jnp.float32) + term_s[d]).astype(jnp.bfloat16)
            remote(4 + d, slot, relay_s.at[d], got_s.at[slot, 4 + d], to).start()

    def local(p, h):
        return pltpu.make_async_copy(fin_s.at[h], y.at[at_rows(p), at_cols(2 * me + h)], l_sem.at[h])

    def finish(p):
        slot = lax.rem(p, 2)

        @pl.when(p >= 1)
        def _():
            for kind in range(6, 10):
                small(kind, slot).wait_send()
            for h in range(2):
                local(p - 1, h).wait()

        for h, (one, two) in enumerate(((4, 3), (2, 5))):
            small(one, slot).wait_recv()
            small(two, slot).wait_recv()
            load_xr(p, h).wait()
            total = term_s[2 + h] + got_s[slot, one].astype(jnp.float32) + got_s[slot, two].astype(jnp.float32)
            fin_s[h] = (xr_s[h].astype(jnp.float32) + total).astype(jnp.bfloat16)
            to_near, to_far = (right, left) if h == 0 else (left, right)
            mine = y.at[at_rows(p), at_cols(2 * me + h)]
            remote(6 + h, slot, fin_s.at[h], mine, to_near).start()
        for h in range(2):
            mine = y.at[at_rows(p), at_cols(2 * me + h)]
            remote(9 - h, slot, fin_s.at[h], mine, left if h == 0 else right).start()
            local(p, h).start()

        @pl.when(p + 1 < chunks)
        def _():
            for h in range(2):
                load_xr(p + 1, h).start()

    def forward(p):
        slot = lax.rem(p, 2)

        @pl.when(p >= 1)
        def _():
            for kind in (10, 11):
                small(kind, slot).wait_send()

        for d, (owner, to) in enumerate(((left, right), (right, left))):
            small(6 + d, slot).wait_recv()
            here = y.at[at_rows(p), at_cols(2 * owner + d)]
            remote(10 + d, slot, here, here, to).start()

    load_x(0).start()
    load_q(0, 0).start()
    load_q(1, 1).start()
    load_cs(0).start()
    for h in range(2):
        load_xr(0, h).start()
    barrier = pltpu.get_barrier_semaphore()
    for to in (left, right):
        pl.semaphore_signal(barrier, inc=1, device_id={"tp": to}, device_id_type=pl.DeviceIdType.MESH)
    pl.semaphore_wait(barrier, 2)

    def period(p, _):
        @pl.when((p >= 0) & (p < chunks))
        def _():
            send_terms(p)

        @pl.when(p >= 1)
        def _():
            finish(p - 1)

        @pl.when((p >= 0) & (p < chunks))
        def _():
            keep_terms(p)

        @pl.when(p + 1 < chunks)
        def _():
            project_first(p + 1)

        @pl.when(p < 0)
        def _():
            for m in range(4):
                load_wo(sent_half(m)).start()
            for m in range(4):
                load_wo(kept_half(m)).start()

        @pl.when((p >= 0) & (p < chunks))
        def _():
            relay(p)

        @pl.when(p + 1 < chunks)
        def _():
            project_rest(p + 1)

        @pl.when(p >= 1)
        def _():
            forward(p - 1)

        @pl.when(p + 1 < chunks)
        def _():
            attention(p + 1)

        return None

    lax.fori_loop(-1, chunks + 1, period, None)
    for p in (chunks - 2, chunks - 1):
        for kind in range(8, 12):
            small(kind, p % 2).wait_recv()
    for kind in range(12):
        small(kind, 0).wait_send()
    for h in range(2):
        local(chunks - 1, h).wait()


def solution(mesh):
    def step(x, gain, wq, wk, wv, wo):
        rows, depth = x.shape
        heads, kv = wq.shape[1] // HEAD, wk.shape[1] // HEAD
        width = depth // (2 * RING)
        half = HEAD // 2
        angle = jnp.arange(rows).astype(jnp.float32)[:, None] * THETA ** (-jnp.arange(half, dtype=jnp.float32) / half)
        cos, sin = jnp.cos(angle), jnp.sin(angle)
        cs = jnp.stack([jnp.concatenate([cos, cos], -1), jnp.concatenate([-sin, sin], -1)])
        any_, vmem = pl.BlockSpec(memory_space=pl.ANY), pl.BlockSpec(memory_space=pltpu.VMEM)
        low, wide = jnp.bfloat16, jnp.float32
        dma = pltpu.SemaphoreType.DMA
        return pl.pallas_call(
            _layer,
            out_shape=jax.ShapeDtypeStruct((rows, depth), low),
            in_specs=[any_, vmem, any_, any_, any_, any_, any_],
            out_specs=any_,
            scratch_shapes=[
                pltpu.VMEM((T, depth), low),
                pltpu.VMEM((T, depth), low),
                pltpu.VMEM((2, T, HEAD), wide),
                pltpu.VMEM((2, depth, WB), low),
                pltpu.VMEM((2 * RING, heads * HEAD, width), low),
                pltpu.VMEM((heads, T, HEAD), low),
                pltpu.VMEM((rows // T, kv, T, HEAD), low),
                pltpu.VMEM((rows // T, kv, HEAD + 16, T), low),
                pltpu.VMEM((T, heads * HEAD), low),
                pltpu.VMEM((heads, T), wide),
                pltpu.VMEM((heads, HEAD + 16, T), wide),
                pltpu.VMEM((4, T, width), low),
                pltpu.VMEM((2, T, width), low),
                pltpu.VMEM((2, T, width), low),
                pltpu.VMEM((2, 6, T, width), low),
                pltpu.VMEM((4, T, width), wide),
                pltpu.VMEM((2, T, width), low),
                dma,
                dma,
                dma((2,)),
                dma((2 * RING,)),
                dma((2,)),
                dma((2,)),
                dma((12,)),
                dma((2, 12)),
            ],
            compiler_params=pltpu.CompilerParams(collective_id=0, has_side_effects=True, vmem_limit_bytes=VMEM),
        )(x, gain.reshape(1, depth), cs, wq, wk, wv, wo)

    tokens, columns = P("dp", None), P(None, "tp")
    return jax.shard_map(
        step,
        mesh=mesh,
        in_specs=(tokens, P(None), columns, columns, columns, P("tp", None)),
        out_specs=tokens,
        check_vma=False,
    )
```

```python
import functools

import jax
import jax.numpy as jnp
from jax import lax
from jax.experimental import pallas as pl
from jax.experimental.pallas import tpu as pltpu
from jax.sharding import PartitionSpec as P

HEAD = 128
THETA = 10000
T = 256
WB = 256
NEG = -1e30
HIDDEN = 2 * NEG
LOG2E = 1.4426950408889634
VMEM = 67_000_000
RING = 4
PARTS = 4
SLOTS = 3
X_PARTS = 4
NORM = 1024
COPY = 64
EARLY = 0.55


def _dot(a, b, ca, cb):
    return lax.dot_general(a, b, (((ca,), (cb,)), ((), ())), preferred_element_type=jnp.float32)


def _layer(x, gain, wq, wk, wv, wo, y, own_0, own_1, a_s, cs_s, w_s, wo_s, q_s, k_s, v_s, seen_s, top_s, mix_s, out_s, relay_s, fin_s, got_s,
           term_s, xr_s, gain_s, x_sem, w_sem, wo_sem, xr_sem, l_sem, s_sem, r_sem):
    rows, depth = x.shape
    chunks = rows // T
    heads, kv = q_s.shape[0], k_s.shape[1]
    group = heads // kv
    width = wo_s.shape[2]
    nq = wq.shape[1] // WB
    nb = nq + 2
    first = (nb + 1) // 2
    half = HEAD // 2
    me = lax.axis_index("tp")
    right, left = lax.rem(me + 1, RING), lax.rem(me + 3, RING)

    def at_rows(p):
        return pl.ds(pl.multiple_of(p * T, T), T)

    def at_cols(hp):
        return pl.ds(pl.multiple_of(hp * width, 128), width)

    def remote(kind, slot, src, dst, to):
        return pltpu.make_async_remote_copy(src_ref=src, dst_ref=dst, send_sem=s_sem.at[kind], recv_sem=r_sem.at[slot, kind],
                                            device_id={"tp": to}, device_id_type=pl.DeviceIdType.MESH)

    def small(kind, slot):
        return remote(kind, slot, out_s.at[0], got_s.at[0, 0], right)

    def load_x(p, i):
        part = T // X_PARTS
        return pltpu.make_async_copy(x.at[pl.ds(pl.multiple_of(p * T + i * part, part), part), :], a_s.at[pl.ds(i * part, part), :], x_sem.at[i])

    def load_xr(p, h):
        return pltpu.make_async_copy(x.at[at_rows(p), at_cols(2 * me + h)], xr_s.at[h], xr_sem.at[h])

    def start_w(w, b, slot):
        for i in range(PARTS):
            part = pl.ds(i * (depth // PARTS), depth // PARTS)
            pltpu.make_async_copy(w.at[part, pl.ds(pl.multiple_of(b * WB, WB), WB)], w_s.at[slot, part], w_sem.at[slot]).start()

    def wait_w(slot):
        pltpu.make_async_copy(wk, w_s.at[slot], w_sem.at[slot]).wait()

    def load_wo(hp):
        return pltpu.make_async_copy(wo.at[:, at_cols(hp)], wo_s.at[hp], wo_sem.at[hp])

    def sent_half(m):
        off = 2 + (m // 2) * (2 * (m % 2) - 1)
        return 2 * lax.rem(me + off, RING) + lax.rem(m % 2 + m // 2, 2)

    def kept_half(m):
        off = (1 - m // 2) * (1 + 2 * (m % 2))
        return 2 * lax.rem(me + off, RING) + m % 2

    def norm(i):
        lanes = depth // (depth // NORM)

        def some(r, _):
            here = pl.ds(pl.multiple_of(i * (T // X_PARTS) + r * 16, 16), 16)
            total = jnp.zeros((16, lanes), jnp.float32)
            for n in range(depth // lanes):
                wide = a_s[here, n * lanes : (n + 1) * lanes].astype(jnp.float32)
                total += wide * wide
            scale = lax.rsqrt(jnp.sum(total, -1, keepdims=True) / depth + 1e-6)
            for n in range(depth // lanes):
                at = slice(n * lanes, (n + 1) * lanes)
                a_s[here, at] = (a_s[here, at].astype(jnp.float32) * scale * gain_s[:, at]).astype(jnp.bfloat16)
            return None

        lax.fori_loop(0, T // X_PARTS // 16, some, None)

    def project(slot):
        wait_w(slot)
        return _dot(a_s[...], w_s[slot], 1, 0).astype(jnp.bfloat16)

    def turn(t):
        wide = t.astype(jnp.float32)
        return (wide * cs_s[0] + pltpu.roll(wide, HEAD // 2, 1) * cs_s[1]).astype(jnp.bfloat16)

    def queries(c):
        def block(b, _):
            slot = lax.rem(c * nb + b, SLOTS)
            t = project(slot)
            for i in range(WB // HEAD):
                q_s[b * (WB // HEAD) + i] = turn(t[:, i * HEAD : (i + 1) * HEAD])

            @pl.when(b + SLOTS < nq)
            def _():
                start_w(wq, b + SLOTS, slot)

            @pl.when(b + SLOTS == nq)
            def _():
                start_w(wk, 0, slot)

            @pl.when(b + SLOTS == nq + 1)
            def _():
                start_w(wv, 0, slot)

            @pl.when((b + SLOTS == nb) & (c >= 1) & (c + 1 < chunks))
            def _():
                start_w(wq, 0, slot)

            return None

        return block

    def tables(c):
        lane = lax.broadcasted_iota(jnp.int32, (T, HEAD), 1)
        at = lane % half
        turns = (c * T + lax.broadcasted_iota(jnp.int32, (T, HEAD), 0)).astype(jnp.float32)
        rate = jnp.ones((T, HEAD), jnp.float32)
        for i in range(half.bit_length() - 1):
            rate = jnp.where((at >> i) % 2 == 1, rate * (THETA ** -(2**i / half)), rate)
        angle = turns * rate
        cs_s[0] = jnp.cos(angle)
        sin = jnp.sin(angle)
        cs_s[1] = jnp.where(lane < half, -sin, sin)

    def project_first(c):
        tables(c)
        for i in range(X_PARTS):
            load_x(c, i).wait()
            norm(i)
        lax.fori_loop(0, first, queries(c), None)

    def start_early(b, slot):
        if b < nq:
            start_w(wq, b, slot)
        else:
            start_w(wk, 0, slot)

    def next_w(c, b, slot):
        @pl.when((c >= 1) & (c + 1 < chunks))
        def _():
            start_early(b, slot)

    def project_rest(c):
        lax.fori_loop(first, nq, queries(c), None)
        slot = lax.rem(c * nb + nq, SLOTS)
        t = project(slot)
        for i in range(kv):
            k_s[c, i] = turn(t[:, i * HEAD : (i + 1) * HEAD])

        next_w(c, 1, slot)
        slot = lax.rem(c * nb + nq + 1, SLOTS)
        t = project(slot)
        for i in range(kv):
            v_s[c, i, :HEAD, :] = t[:, i * HEAD : (i + 1) * HEAD].T
            v_s[c, i, HEAD:, :] = jnp.ones((v_s.shape[2] - HEAD, T), jnp.bfloat16)

        next_w(c, 2, slot)

        @pl.when(c + 1 < chunks)
        def _():
            for i in range(X_PARTS):
                load_x(c + 1, i).start()

    def attention(c):
        e = HEAD**-0.5 * LOG2E
        top_s[...] = jnp.full(top_s.shape, NEG, jnp.float32)
        mix_s[...] = jnp.zeros(mix_s.shape, jnp.float32)
        ok = lax.broadcasted_iota(jnp.int32, (T, T), 0) <= lax.broadcasted_iota(jnp.int32, (T, T), 1)

        def block(j, masked):
            for i in range(kv):
                mine = range(i * group, (i + 1) * group)
                scores = [_dot(k_s[j, i], q_s[h], 1, 1) for h in mine]
                weights, keeps = [], []
                for h, s in zip(mine, scores):
                    if masked:
                        s = jnp.where(ok, s, HIDDEN)
                    old = top_s[h : h + 1, :]
                    top = jnp.maximum(old, s.max(axis=0, keepdims=True))
                    top_s[h : h + 1, :] = top
                    weights.append(jnp.exp2((s - top) * e).astype(jnp.bfloat16))
                    keeps.append(jnp.exp2((old - top) * e))
                for h, p, keep in zip(mine, weights, keeps):
                    mix_s[h] = mix_s[h] * keep + _dot(v_s[j, i], p, 1, 0)

        def whole(j, _):
            block(j, False)
            return None

        lax.fori_loop(0, c, whole, None)
        block(c, True)
        for h in range(heads):
            seen_s[:, h * HEAD : (h + 1) * HEAD] = (mix_s[h, :HEAD, :] * (1 / mix_s[h, HEAD : HEAD + 1, :])).T.astype(jnp.bfloat16)

    def term(p, hp):
        @pl.when(p == 0)
        def _():
            load_wo(hp).wait()

        return _dot(seen_s[...], wo_s[hp], 1, 0)

    def send_terms(p):
        slot = lax.rem(p, 2)

        def one(m, _):
            @pl.when(p >= 1)
            def _():
                small(m, slot).wait_send()

            out_s[m] = term(p, sent_half(m)).astype(jnp.bfloat16)
            remote(m, slot, out_s.at[m], got_s.at[slot, m], lax.rem(me + 1 + 2 * (m % 2), RING)).start()
            return None

        lax.fori_loop(0, 4, one, None)

    def keep_terms(p):
        def one(m, _):
            term_s[m] = term(p, kept_half(m))
            return None

        lax.fori_loop(0, 4, one, None)

    def relay(p):
        slot = lax.rem(p, 2)

        @pl.when(p >= 2)
        def _():
            for kind in range(8, 12):
                small(kind, slot).wait_recv()

        for d, to in ((0, right), (1, left)):

            @pl.when(p >= 1)
            def _():
                small(4 + d, slot).wait_send()

            small(d, slot).wait_recv()
            relay_s[d] = (got_s[slot, d].astype(jnp.float32) + term_s[d]).astype(jnp.bfloat16)
            remote(4 + d, slot, relay_s.at[d], got_s.at[slot, 4 + d], to).start()

    def local(p, h):
        return pltpu.make_async_copy(fin_s.at[h], y.at[at_rows(p), at_cols(2 * me + h)], l_sem.at[h])

    def last(h):
        return pltpu.make_async_copy(fin_s.at[h], (own_0, own_1)[h], l_sem.at[h])

    def finish(p):
        slot = lax.rem(p, 2)

        @pl.when(p >= 1)
        def _():
            for kind in range(6, 10):
                small(kind, slot).wait_send()
            for h in range(2):
                local(p - 1, h).wait()

        for h, (one, two) in enumerate(((4, 3), (2, 5))):
            small(one, slot).wait_recv()
            small(two, slot).wait_recv()
            load_xr(p, h).wait()
            total = term_s[2 + h] + got_s[slot, one].astype(jnp.float32) + got_s[slot, two].astype(jnp.float32)
            fin_s[h] = (xr_s[h].astype(jnp.float32) + total).astype(jnp.bfloat16)
            to_near, to_far = (right, left) if h == 0 else (left, right)
            mine = y.at[at_rows(p), at_cols(2 * me + h)]

            @pl.when(p < chunks - 1)
            def _():
                remote(6 + h, slot, fin_s.at[h], mine, to_near).start()

        @pl.when(p < chunks - 1)
        def _():
            for h in range(2):
                mine = y.at[at_rows(p), at_cols(2 * me + h)]
                remote(9 - h, slot, fin_s.at[h], mine, left if h == 0 else right).start()
                local(p, h).start()

        @pl.when(p == chunks - 1)
        def _():
            for h in range(2):
                last(h).start()

        @pl.when(p + 1 < chunks)
        def _():
            for h in range(2):
                load_xr(p + 1, h).start()

    def forward(p):
        slot = lax.rem(p, 2)

        @pl.when(p >= 1)
        def _():
            for kind in (10, 11):
                small(kind, slot).wait_send()

        for d, (owner, to) in enumerate(((left, right), (right, left))):
            small(6 + d, slot).wait_recv()
            here = y.at[at_rows(p), at_cols(2 * owner + d)]
            remote(10 + d, slot, here, here, to).start()

    for i in range(X_PARTS):
        load_x(0, i).start()
    for b in range(SLOTS):
        start_early(b, b)
    for h in range(2):
        load_xr(0, h).start()
    gain_s[...] = gain[...].astype(jnp.float32).reshape(1, depth)
    barrier = pltpu.get_barrier_semaphore()
    for to in (left, right):
        pl.semaphore_signal(barrier, inc=1, device_id={"tp": to}, device_id_type=pl.DeviceIdType.MESH)

    def period(p, _):
        @pl.when((p >= 0) & (p < chunks))
        def _():
            @pl.when(p == 0)
            def _():
                pl.semaphore_wait(barrier, 2)

            send_terms(p)

        if chunks > 1:

            @pl.when(p == 0)
            def _():
                for b in range(SLOTS):
                    start_early(b, (nb + b) % SLOTS)

        @pl.when(p >= 1)
        def _():
            finish(p - 1)

        @pl.when((p >= 0) & (p < chunks))
        def _():
            keep_terms(p)

        @pl.when(p + 1 < chunks)
        def _():
            project_first(p + 1)

        @pl.when(p < 0)
        def _():
            for m in range(2):
                load_wo(sent_half(m)).start()

        @pl.when((p >= 0) & (p < chunks))
        def _():
            relay(p)

        @pl.when(p + 1 < chunks)
        def _():
            project_rest(p + 1)

        @pl.when(p < 0)
        def _():
            for m in range(2, 4):
                load_wo(sent_half(m)).start()
            for m in range(4):
                load_wo(kept_half(m)).start()

        @pl.when((p >= 1) & (p < chunks))
        def _():
            forward(p - 1)

        @pl.when(p + 1 < chunks)
        def _():
            attention(p + 1)

        return None

    lax.fori_loop(-1, chunks + 1, period, None)
    for kind in range(8, 12):
        small(kind, (chunks - 2) % 2).wait_recv()
    for kind in (0, 1, 2, 3, 4, 5, 10, 11):
        small(kind, 0).wait_send()
    for h in range(2):
        last(h).wait()


def _copy(src, *rest, first, blocks):
    dst, buf, in_sem, out_sem = rest[-4:]
    slots = buf.shape[0]

    def rows(i):
        return pl.ds((first + i) * COPY, COPY)

    def read(i):
        return pltpu.make_async_copy(src.at[rows(i), :], buf.at[i % slots], in_sem.at[i % slots])

    def write(i):
        return pltpu.make_async_copy(buf.at[i % slots], dst.at[rows(i), :], out_sem.at[i % slots])

    for i in range(min(slots, blocks)):
        read(i).start()
    for i in range(blocks + slots // 2):
        if i < blocks:
            read(i).wait()
            write(i).start()
        j = i - slots // 2
        if 0 <= j:
            write(j).wait()
            if j + slots < blocks:
                read(j + slots).start()


def copied(y, first, blocks, onto=None, after=()):
    any_ = pl.BlockSpec(memory_space=pl.ANY)
    given = (y,) + (() if onto is None else (onto,)) + tuple(after)
    return pl.pallas_call(
        functools.partial(_copy, first=first, blocks=blocks),
        out_shape=jax.ShapeDtypeStruct(y.shape, y.dtype),
        in_specs=[any_] * len(given),
        out_specs=any_,
        scratch_shapes=[pltpu.VMEM((8, COPY, y.shape[1]), y.dtype), pltpu.SemaphoreType.DMA((8,)), pltpu.SemaphoreType.DMA((8,))],
        input_output_aliases={} if onto is None else {1: 0},
        compiler_params=pltpu.CompilerParams(vmem_limit_bytes=40 * 2**20),
        cost_estimate=pl.CostEstimate(flops=blocks * 1_000_000_000, bytes_accessed=2 * blocks * COPY * y.shape[1] * 2, transcendentals=0),
    )(*given)


def gathered(y, own_0, own_1):
    rows, depth = y.shape
    width = own_0.shape[1]
    me = lax.axis_index("tp")
    to_right = [(i, (i + 1) % RING) for i in range(RING)]
    to_left = [(i, (i + 3) % RING) for i in range(RING)]
    left_0 = lax.ppermute(own_0, "tp", to_right)
    right_1 = lax.ppermute(own_1, "tp", to_left)
    blocks = (rows - T) // COPY
    some = int(blocks * EARLY)
    out = copied(y, 0, some)
    own_0, own_1, left_0, right_1 = lax.optimization_barrier((own_0, own_1, left_0, right_1))
    far_0 = lax.ppermute(left_0, "tp", to_right)
    far_1 = lax.ppermute(right_1, "tp", to_left)
    left_1 = lax.ppermute(own_1, "tp", to_right)
    right_0 = lax.ppermute(own_0, "tp", to_left)
    out = copied(y, some, blocks - some, out, (left_0, right_1))
    for off, pair in ((0, (own_0, own_1)), (3, (left_0, left_1)), (1, (right_0, right_1)), (2, (far_0, far_1))):
        for h, piece in enumerate(pair):
            out = lax.dynamic_update_slice(out, piece, (rows - T, (2 * lax.rem(me + off, RING) + h) * width))
    return out


def solution(mesh):
    def step(x, gain, wq, wk, wv, wo):
        rows, depth = x.shape
        heads, kv = wq.shape[1] // HEAD, wk.shape[1] // HEAD
        width = depth // (2 * RING)
        any_, vmem = pl.BlockSpec(memory_space=pl.ANY), pl.BlockSpec(memory_space=pltpu.VMEM)
        low, wide = jnp.bfloat16, jnp.float32
        dma = pltpu.SemaphoreType.DMA
        y, own_0, own_1 = pl.pallas_call(
            _layer,
            out_shape=[jax.ShapeDtypeStruct(s, low) for s in ((rows, depth), (T, width), (T, width))],
            in_specs=[any_, vmem, any_, any_, any_, any_],
            out_specs=[any_] * 3,
            scratch_shapes=[
                pltpu.VMEM((T, depth), low),
                pltpu.VMEM((2, T, HEAD), wide),
                pltpu.VMEM((SLOTS, depth, WB), low),
                pltpu.VMEM((2 * RING, heads * HEAD, width), low),
                pltpu.VMEM((heads, T, HEAD), low),
                pltpu.VMEM((rows // T, kv, T, HEAD), low),
                pltpu.VMEM((rows // T, kv, HEAD + 16, T), low),
                pltpu.VMEM((T, heads * HEAD), low),
                pltpu.VMEM((heads, T), wide),
                pltpu.VMEM((heads, HEAD + 16, T), wide),
                pltpu.VMEM((4, T, width), low),
                pltpu.VMEM((2, T, width), low),
                pltpu.VMEM((2, T, width), low),
                pltpu.VMEM((2, 6, T, width), low),
                pltpu.VMEM((4, T, width), wide),
                pltpu.VMEM((2, T, width), low),
                pltpu.VMEM((1, depth), wide),
                dma((X_PARTS,)),
                dma((SLOTS,)),
                dma((2 * RING,)),
                dma((2,)),
                dma((2,)),
                dma((12,)),
                dma((2, 12)),
            ],
            compiler_params=pltpu.CompilerParams(collective_id=0, has_side_effects=True, vmem_limit_bytes=VMEM),
        )(x, gain, wq, wk, wv, wo)
        return gathered(y, own_0, own_1)

    tokens, columns = P("dp", None), P(None, "tp")
    return jax.shard_map(
        step,
        mesh=mesh,
        in_specs=(tokens, P(None), columns, columns, columns, P("tp", None)),
        out_specs=tokens,
        check_vma=False,
    )
```

```python
import functools

import jax
import jax.numpy as jnp
from jax import lax
from jax.experimental import pallas as pl
from jax.experimental.pallas import tpu as pltpu
from jax.sharding import PartitionSpec as P

HEAD = 128
THETA = 10000
T = 256
WB = 256
NEG = -1e30
HIDDEN = 2 * NEG
LOG2E = 1.4426950408889634
VMEM = 67_000_000
RING = 4
PARTS = 4
SLOTS = 3
X_PARTS = 4
NORM = 1024
COPY = 64
FLIGHT = 16


def _dot(a, b, ca, cb):
    return lax.dot_general(a, b, (((ca,), (cb,)), ((), ())), preferred_element_type=jnp.float32)


def _layer(x, gain, wq, wk, wv, wo, y, own_0, own_1, left_0, right_1, a_s, cs_s, w_s, wo_s, q_s, k_s, v_s, seen_s, top_s, mix_s, out_s, relay_s, fin_s, got_s,
           term_s, xr_s, gain_s, x_sem, w_sem, wo_sem, xr_sem, l_sem, s_sem, r_sem):
    rows, depth = x.shape
    chunks = rows // T
    heads, kv = q_s.shape[0], k_s.shape[1]
    group = heads // kv
    width = wo_s.shape[2]
    nq = wq.shape[1] // WB
    nb = nq + 2
    first = (nb + 1) // 2
    half = HEAD // 2
    me = lax.axis_index("tp")
    right, left = lax.rem(me + 1, RING), lax.rem(me + 3, RING)

    def at_rows(p):
        return pl.ds(pl.multiple_of(p * T, T), T)

    def at_cols(hp):
        return pl.ds(pl.multiple_of(hp * width, 128), width)

    def remote(kind, slot, src, dst, to):
        return pltpu.make_async_remote_copy(src_ref=src, dst_ref=dst, send_sem=s_sem.at[kind], recv_sem=r_sem.at[slot, kind],
                                            device_id={"tp": to}, device_id_type=pl.DeviceIdType.MESH)

    def small(kind, slot):
        return remote(kind, slot, out_s.at[0], got_s.at[0, 0], right)

    def load_x(p, i):
        part = T // X_PARTS
        return pltpu.make_async_copy(x.at[pl.ds(pl.multiple_of(p * T + i * part, part), part), :], a_s.at[pl.ds(i * part, part), :], x_sem.at[i])

    def load_xr(p, h):
        return pltpu.make_async_copy(x.at[at_rows(p), at_cols(2 * me + h)], xr_s.at[h], xr_sem.at[h])

    def start_w(w, b, slot):
        for i in range(PARTS):
            part = pl.ds(i * (depth // PARTS), depth // PARTS)
            pltpu.make_async_copy(w.at[part, pl.ds(pl.multiple_of(b * WB, WB), WB)], w_s.at[slot, part], w_sem.at[slot]).start()

    def wait_w(slot):
        pltpu.make_async_copy(wk, w_s.at[slot], w_sem.at[slot]).wait()

    def load_wo(hp):
        return pltpu.make_async_copy(wo.at[:, at_cols(hp)], wo_s.at[hp], wo_sem.at[hp])

    def sent_half(m):
        off = 2 + (m // 2) * (2 * (m % 2) - 1)
        return 2 * lax.rem(me + off, RING) + lax.rem(m % 2 + m // 2, 2)

    def kept_half(m):
        off = (1 - m // 2) * (1 + 2 * (m % 2))
        return 2 * lax.rem(me + off, RING) + m % 2

    def norm(i):
        lanes = depth // (depth // NORM)

        def some(r, _):
            here = pl.ds(pl.multiple_of(i * (T // X_PARTS) + r * 16, 16), 16)
            total = jnp.zeros((16, lanes), jnp.float32)
            for n in range(depth // lanes):
                wide = a_s[here, n * lanes : (n + 1) * lanes].astype(jnp.float32)
                total += wide * wide
            scale = lax.rsqrt(jnp.sum(total, -1, keepdims=True) / depth + 1e-6)
            for n in range(depth // lanes):
                at = slice(n * lanes, (n + 1) * lanes)
                a_s[here, at] = (a_s[here, at].astype(jnp.float32) * scale * gain_s[:, at]).astype(jnp.bfloat16)
            return None

        lax.fori_loop(0, T // X_PARTS // 16, some, None)

    def project(slot):
        wait_w(slot)
        return _dot(a_s[...], w_s[slot], 1, 0).astype(jnp.bfloat16)

    def turn(t):
        wide = t.astype(jnp.float32)
        return (wide * cs_s[0] + pltpu.roll(wide, HEAD // 2, 1) * cs_s[1]).astype(jnp.bfloat16)

    def queries(c):
        def block(b, _):
            slot = lax.rem(c * nb + b, SLOTS)
            t = project(slot)
            for i in range(WB // HEAD):
                q_s[b * (WB // HEAD) + i] = turn(t[:, i * HEAD : (i + 1) * HEAD])

            @pl.when(b + SLOTS < nq)
            def _():
                start_w(wq, b + SLOTS, slot)

            @pl.when(b + SLOTS == nq)
            def _():
                start_w(wk, 0, slot)

            @pl.when(b + SLOTS == nq + 1)
            def _():
                start_w(wv, 0, slot)

            @pl.when((b + SLOTS == nb) & (c >= 1) & (c + 1 < chunks))
            def _():
                start_w(wq, 0, slot)

            return None

        return block

    def tables(c):
        lane = lax.broadcasted_iota(jnp.int32, (T, HEAD), 1)
        at = lane % half
        turns = (c * T + lax.broadcasted_iota(jnp.int32, (T, HEAD), 0)).astype(jnp.float32)
        rate = jnp.ones((T, HEAD), jnp.float32)
        for i in range(half.bit_length() - 1):
            rate = jnp.where((at >> i) % 2 == 1, rate * (THETA ** -(2**i / half)), rate)
        angle = turns * rate
        cs_s[0] = jnp.cos(angle)
        sin = jnp.sin(angle)
        cs_s[1] = jnp.where(lane < half, -sin, sin)

    def project_first(c):
        tables(c)
        for i in range(X_PARTS):
            load_x(c, i).wait()
            norm(i)
        lax.fori_loop(0, first, queries(c), None)

    def start_early(b, slot):
        if b < nq:
            start_w(wq, b, slot)
        else:
            start_w(wk, 0, slot)

    def next_w(c, b, slot):
        @pl.when((c >= 1) & (c + 1 < chunks))
        def _():
            start_early(b, slot)

    def project_rest(c):
        lax.fori_loop(first, nq, queries(c), None)
        slot = lax.rem(c * nb + nq, SLOTS)
        t = project(slot)
        for i in range(kv):
            k_s[c, i] = turn(t[:, i * HEAD : (i + 1) * HEAD])

        next_w(c, 1, slot)
        slot = lax.rem(c * nb + nq + 1, SLOTS)
        t = project(slot)
        for i in range(kv):
            v_s[c, i, :HEAD, :] = t[:, i * HEAD : (i + 1) * HEAD].T
            v_s[c, i, HEAD:, :] = jnp.ones((v_s.shape[2] - HEAD, T), jnp.bfloat16)

        next_w(c, 2, slot)

        @pl.when(c + 1 < chunks)
        def _():
            for i in range(X_PARTS):
                load_x(c + 1, i).start()

    def attention(c):
        e = HEAD**-0.5 * LOG2E
        top_s[...] = jnp.full(top_s.shape, NEG, jnp.float32)
        mix_s[...] = jnp.zeros(mix_s.shape, jnp.float32)
        ok = lax.broadcasted_iota(jnp.int32, (T, T), 0) <= lax.broadcasted_iota(jnp.int32, (T, T), 1)

        def block(j, masked):
            for i in range(kv):
                mine = range(i * group, (i + 1) * group)
                scores = [_dot(k_s[j, i], q_s[h], 1, 1) for h in mine]
                weights, keeps = [], []
                for h, s in zip(mine, scores):
                    if masked:
                        s = jnp.where(ok, s, HIDDEN)
                    old = top_s[h : h + 1, :]
                    top = jnp.maximum(old, s.max(axis=0, keepdims=True))
                    top_s[h : h + 1, :] = top
                    weights.append(jnp.exp2((s - top) * e).astype(jnp.bfloat16))
                    keeps.append(jnp.exp2((old - top) * e))
                for h, p, keep in zip(mine, weights, keeps):
                    mix_s[h] = mix_s[h] * keep + _dot(v_s[j, i], p, 1, 0)

        def whole(j, _):
            block(j, False)
            return None

        lax.fori_loop(0, c, whole, None)
        block(c, True)
        for h in range(heads):
            seen_s[:, h * HEAD : (h + 1) * HEAD] = (mix_s[h, :HEAD, :] * (1 / mix_s[h, HEAD : HEAD + 1, :])).T.astype(jnp.bfloat16)

    def term(p, hp):
        @pl.when(p == 0)
        def _():
            load_wo(hp).wait()

        return _dot(seen_s[...], wo_s[hp], 1, 0)

    def send_terms(p):
        slot = lax.rem(p, 2)

        def one(m, _):
            @pl.when(p >= 1)
            def _():
                small(m, slot).wait_send()

            out_s[m] = term(p, sent_half(m)).astype(jnp.bfloat16)
            remote(m, slot, out_s.at[m], got_s.at[slot, m], lax.rem(me + 1 + 2 * (m % 2), RING)).start()
            return None

        lax.fori_loop(0, 4, one, None)

    def keep_terms(p):
        def one(m, _):
            term_s[m] = term(p, kept_half(m))
            return None

        lax.fori_loop(0, 4, one, None)

    def relay(p):
        slot = lax.rem(p, 2)

        @pl.when(p >= 2)
        def _():
            for kind in range(8, 12):
                small(kind, slot).wait_recv()

        for d, to in ((0, right), (1, left)):

            @pl.when(p >= 1)
            def _():
                small(4 + d, slot).wait_send()

            small(d, slot).wait_recv()
            relay_s[d] = (got_s[slot, d].astype(jnp.float32) + term_s[d]).astype(jnp.bfloat16)
            remote(4 + d, slot, relay_s.at[d], got_s.at[slot, 4 + d], to).start()

    def local(p, h):
        return pltpu.make_async_copy(fin_s.at[h], y.at[at_rows(p), at_cols(2 * me + h)], l_sem.at[h])

    def last(h):
        return pltpu.make_async_copy(fin_s.at[h], (own_0, own_1)[h], l_sem.at[h])

    def finish(p):
        slot = lax.rem(p, 2)

        @pl.when(p >= 1)
        def _():
            for kind in range(6, 10):
                small(kind, slot).wait_send()
            for h in range(2):
                local(p - 1, h).wait()

        for h, (one, two) in enumerate(((4, 3), (2, 5))):
            small(one, slot).wait_recv()
            small(two, slot).wait_recv()
            load_xr(p, h).wait()
            total = term_s[2 + h] + got_s[slot, one].astype(jnp.float32) + got_s[slot, two].astype(jnp.float32)
            fin_s[h] = (xr_s[h].astype(jnp.float32) + total).astype(jnp.bfloat16)
            to_near, to_far = (right, left) if h == 0 else (left, right)
            mine = y.at[at_rows(p), at_cols(2 * me + h)]

            @pl.when(p < chunks - 1)
            def _():
                remote(6 + h, slot, fin_s.at[h], mine, to_near).start()

        @pl.when(p < chunks - 1)
        def _():
            for h in range(2):
                mine = y.at[at_rows(p), at_cols(2 * me + h)]
                remote(9 - h, slot, fin_s.at[h], mine, left if h == 0 else right).start()
                local(p, h).start()

        @pl.when(p == chunks - 1)
        def _():
            for h in range(2):
                remote(6 + h, slot, fin_s.at[h], (left_0, right_1)[h], (right, left)[h]).start()
            for h in range(2):
                last(h).start()

        @pl.when(p + 1 < chunks)
        def _():
            for h in range(2):
                load_xr(p + 1, h).start()

    def forward(p):
        slot = lax.rem(p, 2)

        @pl.when(p >= 1)
        def _():
            for kind in (10, 11):
                small(kind, slot).wait_send()

        for d, (owner, to) in enumerate(((left, right), (right, left))):
            small(6 + d, slot).wait_recv()
            here = y.at[at_rows(p), at_cols(2 * owner + d)]
            remote(10 + d, slot, here, here, to).start()

    for i in range(X_PARTS):
        load_x(0, i).start()
    for b in range(SLOTS):
        start_early(b, b)
    for h in range(2):
        load_xr(0, h).start()
    gain_s[...] = gain[...].astype(jnp.float32).reshape(1, depth)
    barrier = pltpu.get_barrier_semaphore()
    for to in (left, right):
        pl.semaphore_signal(barrier, inc=1, device_id={"tp": to}, device_id_type=pl.DeviceIdType.MESH)

    def period(p, _):
        @pl.when((p >= 0) & (p < chunks))
        def _():
            @pl.when(p == 0)
            def _():
                pl.semaphore_wait(barrier, 2)

            send_terms(p)

        if chunks > 1:

            @pl.when(p == 0)
            def _():
                for b in range(SLOTS):
                    start_early(b, (nb + b) % SLOTS)

        @pl.when(p >= 1)
        def _():
            finish(p - 1)

        @pl.when((p >= 0) & (p < chunks))
        def _():
            keep_terms(p)

        @pl.when(p + 1 < chunks)
        def _():
            project_first(p + 1)

        @pl.when(p < 0)
        def _():
            for m in range(2):
                load_wo(sent_half(m)).start()

        @pl.when((p >= 0) & (p < chunks))
        def _():
            relay(p)

        @pl.when(p + 1 < chunks)
        def _():
            project_rest(p + 1)

        @pl.when(p < 0)
        def _():
            for m in range(2, 4):
                load_wo(sent_half(m)).start()
            for m in range(4):
                load_wo(kept_half(m)).start()

        @pl.when((p >= 1) & (p < chunks))
        def _():
            forward(p - 1)

        @pl.when(p + 1 < chunks)
        def _():
            attention(p + 1)

        return None

    lax.fori_loop(-1, chunks + 1, period, None)
    for kind in range(8, 12):
        small(kind, (chunks - 2) % 2).wait_recv()
    for kind in (6, 7):
        small(kind, (chunks - 1) % 2).wait_recv()
    for kind in (0, 1, 2, 3, 4, 5, 6, 7, 10, 11):
        small(kind, 0).wait_send()
    for h in range(2):
        last(h).wait()


def _placed(pieces, dst, sem):
    rows, width = dst.shape[0], pieces[0][2].shape[1]
    me = lax.axis_index("tp")
    copies = []
    for n, (off, h, ref) in enumerate(pieces):
        at = pl.ds(pl.multiple_of((2 * lax.rem(me + off, RING) + h) * width, 128), width)
        copies.append(pltpu.make_async_copy(ref, dst.at[pl.ds(rows - T, T), at], sem.at[n]))
    return copies


def _copy(src, dst, buf, in_sem, out_sem):
    slots = buf.shape[0]
    blocks = (src.shape[0] - T) // COPY

    def rows(i):
        return pl.ds(i * COPY, COPY)

    def read(i):
        return pltpu.make_async_copy(src.at[rows(i), :], buf.at[i % slots], in_sem.at[i % slots])

    def write(i):
        return pltpu.make_async_copy(buf.at[i % slots], dst.at[rows(i), :], out_sem.at[i % slots])

    for i in range(min(slots, blocks)):
        read(i).start()
    for i in range(blocks + slots // 2):
        if i < blocks:
            read(i).wait()
            write(i).start()
        j = i - slots // 2
        if 0 <= j:
            write(j).wait()
            if j + slots < blocks:
                read(j + slots).start()


def _fill(own_0, own_1, left_0, left_1, right_0, right_1, far_0, far_1, onto, dst, sem):
    given = ((0, own_0, own_1), (3, left_0, left_1), (1, right_0, right_1), (2, far_0, far_1))
    halves = _placed([(off, h, ref) for off, *pair in given for h, ref in enumerate(pair)], dst, sem)
    for copy in halves:
        copy.start()
    for copy in halves:
        copy.wait()


def gathered(y, own_0, own_1, left_0, right_1):
    to_right = [(i, (i + 1) % RING) for i in range(RING)]
    to_left = [(i, (i + 3) % RING) for i in range(RING)]
    far_0 = lax.ppermute(left_0, "tp", to_right)
    far_1 = lax.ppermute(right_1, "tp", to_left)
    left_1 = lax.ppermute(own_1, "tp", to_right)
    right_0 = lax.ppermute(own_0, "tp", to_left)
    any_, vmem = pl.BlockSpec(memory_space=pl.ANY), pl.BlockSpec(memory_space=pltpu.VMEM)
    out = jax.ShapeDtypeStruct(y.shape, y.dtype)
    dma = pltpu.SemaphoreType.DMA
    moved = pl.pallas_call(
        _copy,
        out_shape=out,
        in_specs=[any_],
        out_specs=any_,
        scratch_shapes=[pltpu.VMEM((FLIGHT, COPY, y.shape[1]), y.dtype), dma((FLIGHT,)), dma((FLIGHT,))],
        compiler_params=pltpu.CompilerParams(vmem_limit_bytes=40 * 2**20),
        cost_estimate=pl.CostEstimate(flops=28_000_000_000, bytes_accessed=2 * y.size * 2, transcendentals=0),
    )(y)
    return pl.pallas_call(
        _fill,
        out_shape=out,
        in_specs=[vmem] * 8 + [any_],
        out_specs=any_,
        scratch_shapes=[dma((8,))],
        input_output_aliases={8: 0},
        compiler_params=pltpu.CompilerParams(vmem_limit_bytes=40 * 2**20),
    )(own_0, own_1, left_0, left_1, right_0, right_1, far_0, far_1, moved)


def solution(mesh):
    def step(x, gain, wq, wk, wv, wo):
        rows, depth = x.shape
        heads, kv = wq.shape[1] // HEAD, wk.shape[1] // HEAD
        width = depth // (2 * RING)
        any_, vmem = pl.BlockSpec(memory_space=pl.ANY), pl.BlockSpec(memory_space=pltpu.VMEM)
        low, wide = jnp.bfloat16, jnp.float32
        dma = pltpu.SemaphoreType.DMA
        done = pl.pallas_call(
            _layer,
            out_shape=[jax.ShapeDtypeStruct(s, low) for s in ((rows, depth),) + ((T, width),) * 4],
            in_specs=[any_, vmem, any_, any_, any_, any_],
            out_specs=[any_] * 5,
            scratch_shapes=[
                pltpu.VMEM((T, depth), low),
                pltpu.VMEM((2, T, HEAD), wide),
                pltpu.VMEM((SLOTS, depth, WB), low),
                pltpu.VMEM((2 * RING, heads * HEAD, width), low),
                pltpu.VMEM((heads, T, HEAD), low),
                pltpu.VMEM((rows // T, kv, T, HEAD), low),
                pltpu.VMEM((rows // T, kv, HEAD + 16, T), low),
                pltpu.VMEM((T, heads * HEAD), low),
                pltpu.VMEM((heads, T), wide),
                pltpu.VMEM((heads, HEAD + 16, T), wide),
                pltpu.VMEM((4, T, width), low),
                pltpu.VMEM((2, T, width), low),
                pltpu.VMEM((2, T, width), low),
                pltpu.VMEM((2, 6, T, width), low),
                pltpu.VMEM((4, T, width), wide),
                pltpu.VMEM((2, T, width), low),
                pltpu.VMEM((1, depth), wide),
                dma((X_PARTS,)),
                dma((SLOTS,)),
                dma((2 * RING,)),
                dma((2,)),
                dma((2,)),
                dma((12,)),
                dma((2, 12)),
            ],
            compiler_params=pltpu.CompilerParams(collective_id=0, has_side_effects=True, vmem_limit_bytes=VMEM),
        )(x, gain, wq, wk, wv, wo)
        return gathered(*done)

    tokens, columns = P("dp", None), P(None, "tp")
    return jax.shard_map(
        step,
        mesh=mesh,
        in_specs=(tokens, P(None), columns, columns, columns, P("tp", None)),
        out_specs=tokens,
        check_vma=False,
    )
```
